32 devices in a mesh: seq: 16 (over z, x, core), grp: 2 (over y).
Axes of the slice: x: 2, y: 2, z: 4, core: 2. Of those that a mesh axis runs over, the one named last changes fastest.
Arguments:
- enc_q: bfloat16 [2048, 2048], P('seq', 'grp'), may hold values from -32 to 32
- enc_k: bfloat16 [2048, 2048], P('seq', 'grp'), may hold values from -32 to 32
- enc_v: bfloat16 [2048, 2048], P('seq', 'grp'), may hold values from -6 to 6
- enc_cot: bfloat16 [2048, 2048], P('seq', 'grp'), may hold values from -1.5 to 1.5
- cross_k: bfloat16 [2048, 2048], P('seq', 'grp'), may hold values from -32 to 32
- cross_v: bfloat16 [2048, 2048], P('seq', 'grp'), may hold values from -6 to 6
- dec_q: bfloat16 [512, 2048], P(('seq', 'grp')), may hold values from -32 to 32
- dec_cot: bfloat16 [512, 2048], P(('seq', 'grp')), may hold values from -1.5 to 1.5
- frame_lengths: int32 [16], replicated, may hold values from 64 to 128
Outputs:
- enc_out: bfloat16 [2048, 2048], P('seq', 'grp')
- enc_dq: bfloat16 [2048, 2048], P('seq', 'grp')
- enc_dk: bfloat16 [2048, 2048], P('seq', 'grp')
- enc_dv: bfloat16 [2048, 2048], P('seq', 'grp')
- dec_out: bfloat16 [512, 2048], P(('seq', 'grp'))
- dec_dq: bfloat16 [512, 2048], P(('seq', 'grp'))
- cross_dk: bfloat16 [2048, 2048], P('seq', 'grp')
- cross_dv: bfloat16 [2048, 2048], P('seq', 'grp')
The draws below stay inside these ranges and needn't reach their ends.
All inputs are finite; a program needn't handle non-finite values.
Results may differ from the reference program's by a relative error of at most 0.04.
Values may be sent and summed in bfloat16 or wider, within the bound.
No kernel may reach another device: no remote copies, remote signals or barrier semaphores. Data moves between devices by JAX's collectives and lax.ppermute only.
A program may use at most 128 MiB of HBM per device.

```python
import jax
import jax.numpy as jnp
from jax import lax

HEADS = 16
HEAD_DIM = 128
REACH = 4
FR_DEV = 128
BLOCKS = 16
FRAMES = 2048
TOKENS = 512


def drawn(key, salt, rows):
    inner = jax.random.fold_in(key, salt)
    return jnp.clip(jax.random.normal(inner, (rows, HEADS * HEAD_DIM), jnp.float32), -6.0, 6.0)


def drawn_queries(key, salt, rows):
    content_operand = drawn(key, salt, rows)
    return content_operand.astype(jnp.bfloat16)


def drawn_keys(key, salt, rows):
    content_operand = drawn(key, salt, rows)
    return content_operand.astype(jnp.bfloat16)


def draw_enc_q(key, part):
    return drawn_queries(key, 1, FRAMES)


def draw_enc_k(key, part):
    return drawn_keys(key, 2, FRAMES)


def draw_cross_k(key, part):
    return drawn_keys(key, 3, FRAMES)


def draw_dec_q(key, part):
    return drawn_queries(key, 4, TOKENS)


def with_ends(array, own_key, least, top_value):
    longest = array.shape.index(max(array.shape))
    spots = []
    for shift in (0, 1):
        where = [jax.random.randint(jax.random.fold_in(own_key, axis), (), 0, length) for axis, length in enumerate(array.shape)]
        where[longest] = (where[longest] + shift) % array.shape[longest]
        spots.append(tuple(where))
    return array.at[spots[0]].set(least).at[spots[1]].set(top_value)


def block_levels(own_key, extent, pieces, smallest, largest):
    loudness = 1.0
    for position, blocks in pieces:
        draws = jax.random.uniform(jax.random.fold_in(jax.random.fold_in(own_key, 6), position), (blocks,), jnp.float32, smallest / len(pieces), largest / len(pieces))
        loudness = loudness * jnp.repeat(jnp.exp(draws), extent[position] // blocks).reshape((-1,) + (1,) * (len(extent) - 1 - position))
    return loudness


def normal_values(own_key, extent, scale, reach, split=(), held_as=jnp.bfloat16):
    drawn = jax.random.normal(own_key, extent, jnp.float32) * scale
    if len(split) > 0:
        drawn = block_levels(own_key, extent, split, -0.22, 0.18) * drawn
    return jnp.clip(drawn, min=-reach, max=reach).astype(held_as)


def setup_inputs(seed: int = 0) -> dict:
    streams_of = jax.random.split(jax.random.key(seed), 10)
    enc_q = draw_enc_q(jax.random.fold_in(streams_of[9], 71), 0)
    enc_k = draw_enc_k(jax.random.fold_in(streams_of[9], 71), 0)
    enc_v = normal_values(streams_of[2], (FRAMES, HEADS * HEAD_DIM), 1.0, 6.0, ((0, 16), (1, 2)))
    enc_cot = normal_values(streams_of[3], (FRAMES, HEADS * HEAD_DIM), 0.25, 1.5, ((0, 16), (1, 2)))
    cross_k = draw_cross_k(jax.random.fold_in(streams_of[9], 71), 0)
    cross_v = normal_values(streams_of[5], (FRAMES, HEADS * HEAD_DIM), 1.0, 6.0, ((0, 16), (1, 2)))
    dec_q = draw_dec_q(jax.random.fold_in(streams_of[9], 71), 0)
    dec_cot = normal_values(streams_of[7], (TOKENS, HEADS * HEAD_DIM), 0.25, 1.5, ((0, 32),))
    frame_lengths = with_ends(jax.random.randint(streams_of[8], (BLOCKS,), FR_DEV // 2, FR_DEV + 1), jax.random.fold_in(streams_of[8], 1), FR_DEV // 2, FR_DEV).astype(jnp.int32)
    return {"enc_q": enc_q, "enc_k": enc_k, "enc_v": enc_v, "enc_cot": enc_cot, "cross_k": cross_k, "cross_v": cross_v, "dec_q": dec_q, "dec_cot": dec_cot, "frame_lengths": frame_lengths}


def lowered_precision_twin(content_operand):
    return lax.optimization_barrier(content_operand.astype(jnp.bfloat16)).astype(jnp.float32)

def windows(blocks):
    padded = jnp.pad(blocks, ((REACH, REACH), (0, 0), (0, 0)))
    return jnp.concatenate([padded[offset:offset + BLOCKS] for offset in range(2 * REACH + 1)], axis=1)

def restore_frames(grads):
    parts = grads.reshape(BLOCKS, 2 * REACH + 1, FR_DEV, HEAD_DIM)
    total = jnp.zeros((BLOCKS + 2 * REACH, FR_DEV, HEAD_DIM), jnp.float32)
    for offset in range(2 * REACH + 1):
        total = total + jnp.pad(parts[:, offset], ((offset, 2 * REACH - offset), (0, 0), (0, 0)))
    return total[REACH:REACH + BLOCKS]

def encoder_head(operands, band_valid):
    query_matrix, keyblock, valueblock, output_tangent = operands
    inverse_sqrt_depth = HEAD_DIM ** (-0.5)
    query_matrix = query_matrix.astype(jnp.float32)
    output_tangent = output_tangent.astype(jnp.float32)
    lookup_operand = windows(keyblock.astype(jnp.float32))
    content_operand = windows(valueblock.astype(jnp.float32))
    attention_logits = jnp.einsum('tyf,taf->tya', query_matrix, lookup_operand) * inverse_sqrt_depth
    mask = band_valid[:, None, :]
    top = lax.optimization_barrier(jnp.max(jnp.where(mask, attention_logits, -1e+30), axis=2, keepdims=True))
    softmax_unnormalized = jnp.where(mask, jnp.exp(attention_logits - top), 0.0)
    total = lax.optimization_barrier(jnp.sum(softmax_unnormalized, axis=2, keepdims=True))
    mixture_dividend = jnp.einsum('hpx,hxm->hpm', lowered_precision_twin(softmax_unnormalized), content_operand)
    output = (mixture_dividend / total).astype(jnp.bfloat16)
    delta = lax.optimization_barrier(jnp.sum(output_tangent * output.astype(jnp.float32), axis=2, keepdims=True))
    attention_probs = softmax_unnormalized / total
    prob_gradient = jnp.einsum('tyf,taf->tya', output_tangent, content_operand)
    similarity_adjoint = lowered_precision_twin(attention_probs * (prob_gradient - delta))
    asker_cotangent_sum = (jnp.einsum('hpx,hxm->hpm', similarity_adjoint, lookup_operand) * inverse_sqrt_depth).astype(jnp.bfloat16)
    key_gradient = restore_frames(jnp.einsum('pox,pof->pxf', similarity_adjoint, query_matrix) * inverse_sqrt_depth).astype(jnp.bfloat16)
    value_gradient = restore_frames(jnp.einsum('pox,pof->pxf', lowered_precision_twin(attention_probs), output_tangent)).astype(jnp.bfloat16)
    return (output, asker_cotangent_sum, key_gradient, value_gradient)

def cross_head(operands, frame_valid):
    query_matrix, keyrow, valuerow, output_tangent = operands
    inverse_sqrt_depth = HEAD_DIM ** (-0.5)
    attention_logits = jnp.dot(query_matrix, keyrow.T, preferred_element_type=jnp.float32) * inverse_sqrt_depth
    mask = frame_valid[None, :]
    top = lax.optimization_barrier(jnp.max(jnp.where(mask, attention_logits, -1e+30), axis=1, keepdims=True))
    softmax_unnormalized = jnp.where(mask, jnp.exp(attention_logits - top), 0.0)
    total = lax.optimization_barrier(jnp.sum(softmax_unnormalized, axis=1, keepdims=True))
    mixture_dividend = jnp.dot(softmax_unnormalized.astype(jnp.bfloat16), valuerow, preferred_element_type=jnp.float32)
    output = (mixture_dividend / total).astype(jnp.bfloat16)
    delta = lax.optimization_barrier(jnp.sum(output_tangent.astype(jnp.float32) * output.astype(jnp.float32), axis=1, keepdims=True))
    attention_probs = softmax_unnormalized / total
    prob_gradient = jnp.dot(output_tangent, valuerow.T, preferred_element_type=jnp.float32)
    similarity_adjoint = (attention_probs * (prob_gradient - delta)).astype(jnp.bfloat16)
    asker_cotangent_sum = (jnp.dot(similarity_adjoint, keyrow, preferred_element_type=jnp.float32) * inverse_sqrt_depth).astype(jnp.bfloat16)
    key_gradient = (jnp.dot(similarity_adjoint.T, query_matrix, preferred_element_type=jnp.float32) * inverse_sqrt_depth).astype(jnp.bfloat16)
    value_gradient = jnp.dot(attention_probs.astype(jnp.bfloat16).T, output_tangent, preferred_element_type=jnp.float32).astype(jnp.bfloat16)
    return (output, asker_cotangent_sum, key_gradient, value_gradient)

def frame_heads(matrix):
    return matrix.reshape(BLOCKS, FR_DEV, HEADS, HEAD_DIM).transpose(2, 0, 1, 3)

def frame_rows(tensor):
    return tensor.transpose(1, 2, 0, 3).reshape(FRAMES, HEADS * HEAD_DIM)

def token_heads(matrix, rows):
    return matrix.reshape(rows, HEADS, HEAD_DIM).transpose(1, 0, 2)

def token_rows(tensor, rows):
    return tensor.transpose(1, 0, 2).reshape(rows, HEADS * HEAD_DIM)

def reference(enc_q, enc_k, enc_v, enc_cot, cross_k, cross_v, dec_q, dec_cot, frame_lengths):
    slots = jnp.arange(FR_DEV, dtype=jnp.int32)
    block_valid = slots[None, :] < frame_lengths[:, None]
    padded_valid = jnp.pad(block_valid, ((REACH, REACH), (0, 0)))
    band_valid = jnp.concatenate([padded_valid[offset:offset + BLOCKS] for offset in range(2 * REACH + 1)], axis=1)
    encoded = lax.map(lambda operands: encoder_head(operands, band_valid), (frame_heads(enc_q), frame_heads(enc_k), frame_heads(enc_v), frame_heads(enc_cot)))
    enc_out, enc_dq, enc_dk, enc_dv = [frame_rows(item) for item in encoded]
    frame_valid = block_valid.reshape(FRAMES)
    crossed = lax.map(lambda operands: cross_head(operands, frame_valid), (token_heads(dec_q, TOKENS), token_heads(cross_k, FRAMES), token_heads(cross_v, FRAMES), token_heads(dec_cot, TOKENS)))
    dec_out = token_rows(crossed[0], TOKENS)
    dec_dq = token_rows(crossed[1], TOKENS)
    cross_dk = token_rows(crossed[2], FRAMES)
    cross_dv = token_rows(crossed[3], FRAMES)
    return (enc_out, enc_dq, enc_dk, enc_dv, dec_out, dec_dq, cross_dk, cross_dv)
```

```python
import functools
import math

import jax
import jax.numpy as jnp
from jax import lax
from jax.experimental import pallas as pl
from jax.experimental.pallas import tpu as pltpu
from jax.sharding import PartitionSpec as P

HEAD_DIM = 128
REACH = 4
SCALE = HEAD_DIM ** (-0.5)
LOG2E = math.log2(math.e)
LOW = jnp.bfloat16
OFF = -1e30


VMEM = pl.BlockSpec(memory_space=pltpu.VMEM)
SMEM = pl.BlockSpec(memory_space=pltpu.SMEM)


def swap(block, mask):
    count = lax.axis_size("seq")
    return lax.ppermute(block, "seq", [(i, i ^ mask) for i in range(count)])


def shift(block, distance):
    count = lax.axis_size("seq")
    route = [(i, i + distance) for i in range(count) if 0 <= i + distance < count]
    return lax.ppermute(block, "seq", route)


def rotate(block, distance):
    count = lax.axis_size("seq")
    return lax.ppermute(block, "seq", [(i, (i + distance) % count) for i in range(count)])


def call(body, outs, scratch=(), flops=1_000_000, **kw):
    return pl.pallas_call(
        body,
        out_shape=outs,
        scratch_shapes=scratch,
        cost_estimate=pl.CostEstimate(flops=flops, bytes_accessed=1_000_000, transcendentals=0),
        **kw,
    )


def columns(index, width):
    return pl.ds(pl.multiple_of(index * width, width), width)


def mm(a, b):
    return jnp.dot(a, b, preferred_element_type=jnp.float32)


def mm_t(a, b):
    return lax.dot_general(a, b, (((1,), (1,)), ((), ())), preferred_element_type=jnp.float32)


def pack_kv(enc_k, enc_v, level, width):
    rows = enc_k.shape[0]

    def body(k_ref, v_ref, *outs):
        slot = lax.axis_index("seq") & (level - 1)
        for r in range(level):
            cols = columns(slot ^ r, width)
            outs[r][0] = k_ref[:, cols]
            outs[r][1] = v_ref[:, cols]

    shape = jax.ShapeDtypeStruct((2, rows, width), LOW)
    return call(body, [shape] * level, in_specs=[VMEM] * 2, out_specs=[VMEM] * level)(enc_k, enc_v)


def pack_rest(enc_q, enc_cot, cross_k, cross_v, level, group, width):
    rows = enc_q.shape[0]
    per = width // HEAD_DIM

    def body(q_ref, c_ref, ck_ref, cv_ref, *outs):
        me = lax.axis_index("seq")
        for r in range(group):
            base = 0
            if r < level:
                slot = (me & (level - 1)) ^ r
                for ref in (q_ref, c_ref):
                    for h in range(per):
                        outs[r][base : base + rows] = ref[:, columns(slot * per + h, HEAD_DIM)]
                        base += rows
            cols = columns((me & (group - 1)) ^ r, HEAD_DIM)
            outs[r][base : base + rows] = ck_ref[:, cols]
            outs[r][base + rows : base + 2 * rows] = cv_ref[:, cols]

    shapes = [
        jax.ShapeDtypeStruct(((2 * per if r < level else 0) * rows + 2 * rows, HEAD_DIM), LOW)
        for r in range(group)
    ]
    return call(body, shapes, in_specs=[VMEM] * 4, out_specs=[VMEM] * group)(
        enc_q, enc_cot, cross_k, cross_v
    )


def pack_tokens(dec_q, dec_cot, count, groups_heads, grp):
    tokens = dec_q.shape[0]

    def body(q_ref, c_ref, out):
        for d in range(count):
            head = (d % grp) * groups_heads + (d // grp) % groups_heads
            cols = slice(head * HEAD_DIM, (head + 1) * HEAD_DIM)
            out[d, 0] = q_ref[:, cols]
            out[d, 1] = c_ref[:, cols]

    shape = jax.ShapeDtypeStruct((count, 2, tokens, HEAD_DIM), LOW)
    return call(body, shape, in_specs=[VMEM] * 2, out_specs=VMEM)(dec_q, dec_cot)


def gather_level(pieces):
    def body(*refs):
        out = refs[-1]
        for r, ref in enumerate(refs[:-1]):
            out[r] = ref[...]

    shape = jax.ShapeDtypeStruct((len(pieces),) + pieces[0].shape, LOW)
    return call(body, shape, in_specs=[VMEM] * len(pieces), out_specs=VMEM)(*pieces)


def encoder(lengths, own, left, right, rest, level, per):
    rows = own.shape[2]
    reach_rows = (2 * REACH + 1) * rows
    total_rows = 3 * level * rows
    blocks = lengths.shape[0]

    def body(len_ref, left_ref, own_ref, right_ref, *refs):
        rest_refs = refs[:level]
        od_refs = refs[level : 2 * level]
        gown, gleft, gright = refs[2 * level : 2 * level + 3]
        ks, vs, kt, vt, bias, dk_acc, dv_acc = refs[2 * level + 3 :]
        head = pl.program_id(0)
        me = lax.axis_index("seq")
        slot = me & (level - 1)
        first = me - slot - level

        @pl.when(head == 0)
        def _():
            row = lax.broadcasted_iota(jnp.int32, (rows, HEAD_DIM), 0)
            for b in range(3 * level):
                block = first + b
                inside = (block >= 0) & (block < blocks)
                length = jnp.where(inside, len_ref[jnp.clip(block, 0, blocks - 1)], 0)
                bias[b * rows : (b + 1) * rows] = jnp.where(row < length, 0.0, OFF)

        for side, ref in enumerate((left_ref, own_ref, right_ref)):
            for r in range(level):
                where = columns(side * level + (slot ^ r), rows)
                kb, vb = ref[r, 0], ref[r, 1]
                ks[where, :] = kb
                vs[where, :] = vb
                kt[:, where] = kb.T
                vt[:, where] = vb.T
        dk_acc[...] = jnp.zeros_like(dk_acc)
        dv_acc[...] = jnp.zeros_like(dv_acc)
        for r in range(level):
            q = rest_refs[r][columns(head, rows), :]
            cot = rest_refs[r][columns(per + head, rows), :]
            span = pl.ds(pl.multiple_of((slot ^ r) * rows, rows), reach_rows)
            kw, vw = ks[span, :], vs[span, :]
            t = mm_t(kw, q) * (SCALE * LOG2E) + bias[span, :]
            top = jnp.max(t, axis=0, keepdims=True)
            e = jnp.exp2(t - top)
            total = jnp.sum(e, axis=0, keepdims=True)
            inv = 1.0 / total
            out_t = mm(vt[:, span], e.astype(LOW)) * inv
            out = out_t.T.astype(LOW)
            cot_t = cot.astype(jnp.float32).T
            delta = jnp.sum(
                cot_t * out_t.astype(LOW).astype(jnp.float32), axis=0, keepdims=True
            )
            p = e * inv
            ds = (p * (mm_t(vw, cot) - delta)).astype(LOW)
            dq = (mm(kt[:, span], ds) * SCALE).T.astype(LOW)
            od_refs[r][0] = out
            od_refs[r][1] = dq
            dk_acc[span, :] += mm(ds, q)
            dv_acc[span, :] += mm(p.astype(LOW), cot)
        for side, ref in enumerate((gleft, gown, gright)):
            for r in range(level):
                where = columns(side * level + (slot ^ r), rows)
                ref[r, 0] = (dk_acc[where, :] * SCALE).astype(ref.dtype)
                ref[r, 1] = dv_acc[where, :].astype(ref.dtype)

    width = per * HEAD_DIM
    kv_spec = pl.BlockSpec((level, 2, rows, HEAD_DIM), lambda h: (0, 0, 0, h))
    od_spec = pl.BlockSpec((2, rows, HEAD_DIM), lambda h: (0, 0, h))
    full = [pl.BlockSpec(x.shape, lambda h: (0, 0)) for x in rest[:level]]
    shapes = [jax.ShapeDtypeStruct((2, rows, width), LOW)] * level + [
        jax.ShapeDtypeStruct((level, 2, rows, width), d) for d in (jnp.float32, LOW, LOW)
    ]
    flat = pltpu.VMEM((total_rows, HEAD_DIM), LOW)
    wide = pltpu.VMEM((HEAD_DIM, total_rows), LOW)
    acc = pltpu.VMEM((total_rows, HEAD_DIM), jnp.float32)
    outs = call(
        body,
        shapes,
        scratch=[flat, flat, wide, wide, acc, acc, acc],
        flops=12 * per * level * rows * reach_rows * HEAD_DIM,
        grid=(per,),
        in_specs=[SMEM] + [kv_spec] * 3 + full,
        out_specs=[od_spec] * level + [kv_spec] * 3,
    )(lengths, left, own, right, *rest[:level])
    return outs[:level], outs[level], outs[level + 1], outs[level + 2]


def add_halo(own, from_left, from_right):
    level = own.shape[0]

    def body(own_ref, l_ref, r_ref, *outs):
        for r in range(level):
            outs[r][...] = (
                own_ref[r] + l_ref[r].astype(jnp.float32) + r_ref[r].astype(jnp.float32)
            ).astype(LOW)

    shape = jax.ShapeDtypeStruct(own.shape[1:], LOW)
    return call(body, [shape] * level, in_specs=[VMEM] * 3, out_specs=[VMEM] * level)(
        own, from_left, from_right
    )


def assemble(pieces, level):
    rows, width = pieces[0].shape[1:]

    def body(*refs):
        slot = lax.axis_index("seq") & (level - 1)
        for r in range(level):
            cols = columns(slot ^ r, width)
            refs[level][:, cols] = refs[r][0]
            refs[level + 1][:, cols] = refs[r][1]

    shape = jax.ShapeDtypeStruct((rows, level * width), LOW)
    return call(body, [shape] * 2, in_specs=[VMEM] * level, out_specs=[VMEM] * 2)(*pieces)


def cross_bias(len_ref, bias, rows, group):
    me = lax.axis_index("seq")
    row = lax.broadcasted_iota(jnp.int32, (rows, HEAD_DIM), 0)
    for r in range(group):
        bias[r * rows : (r + 1) * rows] = jnp.where(row < len_ref[me ^ r], 0.0, OFF)


def load_cross(rest_refs, tok_ref, keys, vals, tq, tc, rows):
    for r, ref in enumerate(rest_refs):
        base = ref.shape[0] - 2 * rows
        keys[r * rows : (r + 1) * rows] = ref[base : base + rows]
        vals[r * rows : (r + 1) * rows] = ref[base + rows : base + 2 * rows]
    count, _, tokens, _ = tok_ref.shape
    for d in range(count):
        tq[d * tokens : (d + 1) * tokens] = tok_ref[d, 0]
        tc[d * tokens : (d + 1) * tokens] = tok_ref[d, 1]


def cross_scratch(group, rows, all_tokens):
    return [
        pltpu.VMEM((group * rows, HEAD_DIM), LOW),
        pltpu.VMEM((group * rows, HEAD_DIM), LOW),
        pltpu.VMEM((all_tokens, HEAD_DIM), LOW),
        pltpu.VMEM((all_tokens, HEAD_DIM), LOW),
        pltpu.VMEM((group * rows, HEAD_DIM), jnp.float32),
    ]


TILE = 128


def cross_stats(lengths, rest, tok, group, rows):
    all_tokens = tok.shape[0] * tok.shape[2]

    def body(len_ref, *refs):
        out = refs[group + 1]
        keys, vals, tq, tc, bias = refs[group + 2 :]
        load_cross(refs[:group], refs[group], keys, vals, tq, tc, rows)
        cross_bias(len_ref, bias, rows, group)
        vals_t = vals[...].T
        out[...] = jnp.zeros_like(out)
        for c in range(all_tokens // TILE):
            part = slice(c * TILE, (c + 1) * TILE)
            t = mm_t(keys[...], tq[part]) * (SCALE * LOG2E) + bias[...]
            top = jnp.max(t, axis=0, keepdims=True)
            e = jnp.exp2(t - top)
            numer = mm(vals_t, e.astype(LOW))
            out[0:1, part] = top
            out[1:2, part] = jnp.sum(e, axis=0, keepdims=True)
            out[2:3, part] = jnp.sum(
                numer * tc[part].astype(jnp.float32).T, axis=0, keepdims=True
            )

    return call(
        body,
        jax.ShapeDtypeStruct((8, all_tokens), jnp.float32),
        scratch=cross_scratch(group, rows, all_tokens),
        flops=4 * group * rows * all_tokens * HEAD_DIM,
        in_specs=[SMEM] + [VMEM] * (group + 1),
        out_specs=VMEM,
    )(lengths, *rest, tok)


def cross_grads(lengths, rest, tok, stats, group, rows):
    all_tokens = tok.shape[0] * tok.shape[2]
    tokens = tok.shape[2]
    others = len(stats)

    def body(len_ref, *refs):
        stat_refs = refs[group + 1 : group + 1 + others]
        refs_out = refs[group + 1 + others :]
        grads, back = refs_out[:group], refs_out[group]
        keys, vals, tq, tc, bias, dk_acc, dv_acc = refs_out[group + 1 :]
        load_cross(refs[:group], refs[group], keys, vals, tq, tc, rows)
        cross_bias(len_ref, bias, rows, group)
        vals_t, keys_t = vals[...].T, keys[...].T
        for c in range(all_tokens // TILE):
            part = slice(c * TILE, (c + 1) * TILE)
            tops = [ref[0:1, part] for ref in stat_refs]
            top = functools.reduce(jnp.maximum, tops)
            weights = [jnp.exp2(x - top) for x in tops]
            total = sum(w * ref[1:2, part] for w, ref in zip(weights, stat_refs))
            inv = 1.0 / total
            delta = sum(w * ref[2:3, part] for w, ref in zip(weights, stat_refs)) * inv
            q, cot = tq[part], tc[part]
            t = mm_t(keys[...], q) * (SCALE * LOG2E) + bias[...]
            e = jnp.exp2(t - top)
            out = (mm(vals_t, e.astype(LOW)) * inv).T.astype(LOW)
            p = e * inv
            ds = (p * (mm_t(vals[...], cot) - delta)).astype(LOW)
            dq = (mm(keys_t, ds) * SCALE).T.astype(LOW)
            for i in range(TILE // tokens):
                back[c * (TILE // tokens) + i, 0] = out[i * tokens : (i + 1) * tokens]
                back[c * (TILE // tokens) + i, 1] = dq[i * tokens : (i + 1) * tokens]
            gk, gv = mm(ds, q), mm(p.astype(LOW), cot)
            if c == 0:
                dk_acc[...], dv_acc[...] = gk, gv
            else:
                dk_acc[...] += gk
                dv_acc[...] += gv
        for r in range(group):
            grads[r][0] = (dk_acc[r * rows : (r + 1) * rows] * SCALE).astype(LOW)
            grads[r][1] = dv_acc[r * rows : (r + 1) * rows].astype(LOW)

    acc = pltpu.VMEM((group * rows, HEAD_DIM), jnp.float32)
    shapes = [jax.ShapeDtypeStruct((2, rows, HEAD_DIM), LOW)] * group
    outs = call(
        body,
        shapes + [jax.ShapeDtypeStruct(tok.shape, LOW)],
        scratch=cross_scratch(group, rows, all_tokens) + [acc, acc],
        flops=12 * group * rows * all_tokens * HEAD_DIM,
        in_specs=[SMEM] + [VMEM] * (group + 1 + others),
        out_specs=[VMEM] * (group + 1),
    )(lengths, *rest, tok, *stats)
    return outs[:group], outs[group]


def finish_tokens(back, heads, grp, group):
    count, _, tokens, _ = back.shape

    def body(ref, out, dq):
        for y in range(grp):
            for m in range(group):
                head = y * group + m
                cols = slice(head * HEAD_DIM, (head + 1) * HEAD_DIM)
                parts = range(m * grp + y, count, group * grp)
                for which, dst in ((0, out), (1, dq)):
                    dst[:, cols] = sum(ref[d, which].astype(jnp.float32) for d in parts).astype(LOW)

    shape = jax.ShapeDtypeStruct((tokens, heads * HEAD_DIM), LOW)
    return call(body, [shape] * 2, in_specs=[VMEM], out_specs=[VMEM] * 2)(back)


def local(enc_q, enc_k, enc_v, enc_cot, cross_k, cross_v, dec_q, dec_cot, lengths):
    count, grp = lax.axis_size("seq"), lax.axis_size("grp")
    rows = enc_q.shape[0]
    group = enc_q.shape[1] // HEAD_DIM
    level = REACH
    per = group // level
    width = per * HEAD_DIM

    tok = pack_tokens(dec_q, dec_cot, count * grp, group, grp)
    kv = pack_kv(enc_k, enc_v, level, width)
    kv = [kv[0]] + [swap(kv[r], r) for r in range(1, level)]
    tok = lax.all_to_all(tok, ("seq", "grp"), 0, 0, tiled=True)
    rest = pack_rest(enc_q, enc_cot, cross_k, cross_v, level, group, width)
    rest = [rest[0]] + [swap(rest[r], r) for r in range(1, group)]
    own = gather_level(kv)
    left = shift(own, level)
    right = shift(own, -level)
    od, gown, gleft, gright = encoder(lengths, own, left, right, rest, level, per)
    from_right = shift(gleft, -level)
    from_left = shift(gright, level)
    od = [od[0]] + [swap(od[r], r) for r in range(1, level)]

    stats = [cross_stats(lengths, rest, tok, group, rows)]
    stats += [rotate(stats[0], k * group) for k in range(1, count // group)]
    grads, back = cross_grads(lengths, rest, tok, stats, group, rows)
    back = lax.all_to_all(back, ("seq", "grp"), 0, 0, tiled=True)
    grads = [grads[0]] + [swap(grads[r], r) for r in range(1, group)]

    enc_out, enc_dq = assemble(od, level)
    gkv = add_halo(gown, from_left, from_right)
    gkv = [gkv[0]] + [swap(gkv[r], r) for r in range(1, level)]
    cross_dk, cross_dv = assemble(grads, group)
    dec_out, dec_dq = finish_tokens(back, grp * group, grp, group)
    enc_dk, enc_dv = assemble(gkv, level)
    return (enc_out, enc_dq, enc_dk, enc_dv, dec_out, dec_dq, cross_dk, cross_dv)


def solution(mesh):
    frames, tokens = P("seq", "grp"), P(("seq", "grp"), None)
    return jax.shard_map(
        local,
        mesh=mesh,
        in_specs=(frames,) * 6 + (tokens, tokens, P()),
        out_specs=(frames,) * 4 + (tokens, tokens, frames, frames),
        check_vma=False,
    )
```
